256 devices in a mesh: occ: 8 (over z), vsec: 16 (over y, x_lo, core), aux: 2 (over x_hi).
Axes of the slice: x: 4 (x_hi: 2, x_lo: 2; x = x_hi * 2 + x_lo), y: 4, z: 8, core: 2. Of those that a mesh axis runs over, the one named last changes fastest.
Arguments:
- amplitudes: bfloat16 [128, 1024, 1024], P(('occ', 'vsec'), 'aux'), may hold values from -0.005859375 to 0.005859375
- left_factor: bfloat16 [4096, 32, 1024], P('aux', 'vsec'), may hold values from -0.75 to 0.75
- right_factor: bfloat16 [4096, 8, 1024], P('aux', None, 'occ'), may hold values from -0.75 to 0.75
- other_terms: float32 [128, 32, 8], P(('occ', 'aux'), 'vsec'), may hold values from -10.4 to 10.4
Outputs:
- residual: float32 [128, 32, 8], P(('occ', 'aux'), 'vsec')
- residual_norm: float32 [], replicated
The draws below stay inside these ranges and needn't reach their ends.
All inputs are finite; a program needn't handle non-finite values.
Results may differ from the reference program's by a relative error of at most 0.002.
Values may be sent and summed in bfloat16 or wider, within the bound.
No kernel may reach another device: no remote copies, remote signals or barrier semaphores. Data moves between devices by JAX's collectives and lax.ppermute only.
A program may use at most 192 MiB of HBM per device.

```python
import jax
import jax.numpy as jnp
from jax import lax

VIRT = 1024
NAUX = 4096
BWIN = 8
PAIRS = 128
AROWS = 32


def draw_other_terms(key, part):
    key_base = jax.random.fold_in(jax.random.fold_in(key, 17), 0)
    pair_pos = jnp.arange(PAIRS, dtype=jnp.float32) / max(PAIRS - 1, 1)
    row_pos = jnp.arange(AROWS, dtype=jnp.float32) / max(AROWS - 1, 1)
    rising = 0.5 * (12.0 ** (0.25 * pair_pos))[:, None, None] * (12.0 ** (0.25 * row_pos))[None, :, None]
    base = jax.random.normal(key_base, (PAIRS, AROWS, BWIN), jnp.float32)
    base = jnp.clip(base, -6.0, 6.0)
    return (base * rising).astype(jnp.float32)


def levels(rng, dims, cuts, least, top_value):
    gain, own = 1.0, jax.random.fold_in(rng, 6)
    for dim, parts in cuts:
        heights = jnp.exp(jax.random.uniform(jax.random.fold_in(own, dim), (parts,), jnp.float32, least / len(cuts), top_value / len(cuts)))
        gain = gain * jnp.repeat(heights, dims[dim] // parts).reshape([-1 if axis == dim else 1 for axis in range(len(dims))])
    return gain


def bell_draw(key, extent, width, reach, cuts=(), held_as=jnp.bfloat16):
    result = width * jax.random.normal(key, extent, jnp.float32)
    if cuts:
        result = result * levels(key, extent, cuts, -0.22, 0.18)
    return jnp.clip(result, -reach, reach).astype(held_as)


def setup_inputs(seed: int = 0) -> dict:
    seeds = jax.random.split(jax.random.key(seed), 5)
    amplitudes = bell_draw(seeds[0], (PAIRS, VIRT, VIRT), (VIRT * VIRT) ** -0.5, 0.005859375, ((0, 128), (1, 2)))
    left_factor = bell_draw(seeds[1], (NAUX, AROWS, VIRT), (NAUX ** 0.5) ** -0.5, 0.75, ((0, 2), (1, 16)))
    right_factor = bell_draw(seeds[2], (NAUX, BWIN, VIRT), (NAUX ** 0.5) ** -0.5, 0.75, ((0, 2), (2, 8)))
    other_terms = draw_other_terms(jax.random.fold_in(seeds[4], 71), 0)
    return {"amplitudes": amplitudes, "left_factor": left_factor, "right_factor": right_factor, "other_terms": other_terms}


def reference(amplitudes, left_factor, right_factor, other_terms):
    pairs_all = amplitudes.shape[0]
    virt_width = amplitudes.shape[1]
    aux_width = left_factor.shape[0]
    window = right_factor.shape[1]
    amp_flat = amplitudes.astype(jnp.float32).reshape(pairs_all, virt_width * virt_width)
    right_flat = right_factor.reshape(aux_width, window * virt_width)
    rows_first = jnp.transpose(left_factor, (1, 0, 2))

    def one_row(row_factor):
        integral = lax.dot_general(row_factor, right_flat, (((0,), (0,)), ((), ())), preferred_element_type=jnp.float32)
        rounded = lax.optimization_barrier(integral.astype(jnp.bfloat16))
        integral = rounded.astype(jnp.float32)
        integral = integral.reshape(virt_width, window, virt_width).transpose(0, 2, 1).reshape(virt_width * virt_width, window)
        return jnp.dot(amp_flat, integral, precision=lax.Precision.HIGHEST, preferred_element_type=jnp.float32)
    ladder = lax.map(one_row, rows_first)
    ladder = jnp.transpose(ladder, (1, 0, 2))
    residual = other_terms + ladder
    residual_norm = jnp.sqrt(jnp.sum(residual * residual))
    return (residual, residual_norm)
```

```python
import jax
import jax.numpy as jnp
from jax import lax
from jax.sharding import Mesh
from jax.sharding import PartitionSpec as P

VSEC = ("vsec_0", "vsec_1", "vsec_2")
PLANE = ("aux",) + VSEC
OCC_VSEC = ("occ",) + VSEC
SCALE = 32.0


def exchange(x, axes):
    return lax.all_to_all(x, axes, split_axis=0, concat_axis=0, tiled=True)


def on_device(amplitudes, left_factor, right_factor, other_terms):
    occ_count = lax.axis_size("occ")
    aux_count = lax.axis_size("aux")
    sec_count = lax.axis_size(VSEC)
    plane_count = aux_count * sec_count
    aux_rows, arow_count, virt_width = left_factor.shape
    window, slice_width = right_factor.shape[1:]
    sub = virt_width // plane_count
    per_device = other_terms.shape[0]

    amps = amplitudes.reshape(sec_count, sub, occ_count, slice_width)
    amps = jnp.transpose(amps, (2, 0, 1, 3)).reshape(occ_count * sec_count, sub, slice_width)
    amps = exchange(amps, OCC_VSEC)

    partial = lax.dot_general(
        left_factor.reshape(aux_rows, arow_count * virt_width),
        right_factor.reshape(aux_rows, window * slice_width),
        (((0,), (0,)), ((), ())),
        preferred_element_type=jnp.float32,
    )
    partial = (partial * SCALE).astype(jnp.float16)
    partial = partial.reshape(arow_count, plane_count, sub, window, slice_width)
    partial = jnp.transpose(partial, (1, 0, 3, 2, 4))
    partial, amps = lax.optimization_barrier((partial, amps))
    arrived = exchange(partial, PLANE)
    halves = arrived.reshape(aux_count, sec_count * arow_count, window, sub, slice_width)
    integral = (halves.astype(jnp.float32).sum(axis=0) * (1.0 / SCALE)).astype(jnp.bfloat16)

    ladder = lax.dot_general(
        amps, integral, (((1, 2), (2, 3)), ((), ())), preferred_element_type=jnp.float32
    )
    ladder = ladder.reshape(occ_count, aux_count, per_device, sec_count, arow_count, window)
    ladder = jnp.transpose(ladder, (1, 3, 0, 2, 4, 5)).reshape(plane_count, -1, 128)
    mine = exchange(ladder, PLANE).sum(axis=0)
    mine = mine.reshape(occ_count, 1, 128)
    place = lax.axis_index("occ")
    slot = lax.broadcasted_iota(jnp.int32, (occ_count, 1, 128), 0)
    mine = mine + jnp.where(slot == place, other_terms.reshape(1, 1, 128), 0.0)
    spread = jnp.broadcast_to(mine.reshape(1, occ_count, 128), (occ_count, occ_count, 128))
    whole = exchange(spread, "occ").sum(axis=0)
    residual = lax.dynamic_slice_in_dim(whole, place, 1, 0).reshape(other_terms.shape)
    square = jnp.sum(whole * whole)
    squares = exchange(jnp.broadcast_to(square, (plane_count, 1, 128)), PLANE)
    norm = jnp.sqrt(jnp.sum(squares[:, 0, 0]))
    return (residual, norm)


def solution(mesh):
    torus = Mesh(
        mesh.devices.reshape(mesh.shape["occ"], 4, 2, 2, mesh.shape["aux"]),
        ("occ", "vsec_0", "vsec_1", "vsec_2", "aux"),
    )
    in_specs = (
        P(OCC_VSEC, "aux", None),
        P("aux", VSEC, None),
        P("aux", None, "occ"),
        P(("occ", "aux"), VSEC, None),
    )
    out_specs = (P(("occ", "aux"), VSEC, None), P())
    return jax.shard_map(
        on_device, mesh=torus, in_specs=in_specs, out_specs=out_specs, check_vma=False
    )
```

```python
import jax
import jax.numpy as jnp
from jax import lax
from jax.sharding import Mesh
from jax.sharding import PartitionSpec as P

VSEC = ("vsec_0", "vsec_1", "vsec_2")
PLANE = ("aux",) + VSEC
OCC_VSEC = ("occ",) + VSEC
OCC_AUX = ("occ", "aux")
SCALE = 32.0


def exchange(x, axes):
    return lax.all_to_all(x, axes, split_axis=0, concat_axis=0, tiled=True)


def spread_slices(rows, count, width):
    own = lax.axis_index("occ")
    whole = jnp.zeros((count, rows.shape[0], width), rows.dtype)
    for step in range(count):
        peer = own ^ step
        piece = lax.dynamic_slice_in_dim(rows, peer * width, width, 1)
        if step:
            piece = lax.ppermute(piece, "occ", [(i, i ^ step) for i in range(count)])
        whole = lax.dynamic_update_index_in_dim(whole, piece, peer, 0)
    return whole


def on_device(amplitudes, left_factor, right_factor, other_terms):
    occ_count = lax.axis_size("occ")
    aux_count = lax.axis_size("aux")
    sec_count = lax.axis_size(VSEC)
    plane_count = aux_count * sec_count
    aux_rows, arow_count, virt_width = left_factor.shape
    window, slice_width = right_factor.shape[1:]
    sub = virt_width // plane_count
    per_device = other_terms.shape[0]

    amps = amplitudes.reshape(sec_count, sub, occ_count * slice_width)
    amps = exchange(amps, VSEC).reshape(sec_count * sub, occ_count * slice_width)

    partial = lax.dot_general(
        left_factor, right_factor, (((0,), (0,)), ((), ())), preferred_element_type=jnp.float32
    )
    partial = (partial * SCALE).astype(jnp.float16)
    partial = partial.reshape(arow_count, plane_count, sub, window, slice_width)
    partial = jnp.transpose(partial, (1, 0, 3, 2, 4))
    partial, amps = lax.optimization_barrier((partial, amps))
    arrived = exchange(partial, PLANE)
    amps = spread_slices(amps, occ_count, slice_width)
    amps = amps.reshape(occ_count * sec_count, sub, slice_width)
    halves = arrived.reshape(aux_count, sec_count * arow_count, window, sub, slice_width)
    total = halves[0].astype(jnp.float32)
    for half in range(1, aux_count):
        total = total + halves[half].astype(jnp.float32)
    integral = (total * (1.0 / SCALE)).astype(jnp.bfloat16)

    ladder = lax.dot_general(
        integral, amps, (((2, 3), (1, 2)), ((), ())), preferred_element_type=jnp.float32
    )
    rows = arow_count * window
    pairs = amps.shape[0]
    mine = exchange(ladder.reshape(sec_count, rows, pairs), VSEC).sum(axis=0)
    place = lax.axis_index(OCC_AUX) * per_device
    others = jnp.transpose(other_terms.reshape(per_device, rows))
    others = lax.dynamic_update_slice(jnp.zeros((rows, pairs), jnp.float32), others, (0, place))
    mine = mine + others
    spread = jnp.broadcast_to(mine, (occ_count * aux_count, rows, pairs))
    whole = exchange(spread, OCC_AUX).sum(axis=0)
    residual = lax.dynamic_slice_in_dim(whole, place, per_device, 1)
    residual = jnp.transpose(residual).reshape(other_terms.shape)
    square = jnp.sum(whole * whole, axis=0)
    squares = exchange(jnp.broadcast_to(square, (sec_count, 1, pairs)), VSEC)
    norm = jnp.sqrt(jnp.sum(squares))
    return (residual, norm)


def solution(mesh):
    torus = Mesh(
        mesh.devices.reshape(mesh.shape["occ"], 4, 2, 2, mesh.shape["aux"]),
        ("occ", "vsec_0", "vsec_1", "vsec_2", "aux"),
    )
    in_specs = (
        P(OCC_VSEC, "aux", None),
        P("aux", VSEC, None),
        P("aux", None, "occ"),
        P(("occ", "aux"), VSEC, None),
    )
    out_specs = (P(("occ", "aux"), VSEC, None), P())
    return jax.shard_map(
        on_device, mesh=torus, in_specs=in_specs, out_specs=out_specs, check_vma=False
    )
```

```python
import jax
import jax.numpy as jnp
from jax import lax
from jax.sharding import Mesh
from jax.sharding import PartitionSpec as P

VSEC = ("vsec_0", "vsec_1", "vsec_2")
PLANE = ("aux",) + VSEC
OCC_VSEC = ("occ",) + VSEC
OCC_AUX = ("occ", "aux")
SCALE = 32.0


def exchange(x, axes):
    return lax.all_to_all(x, axes, split_axis=0, concat_axis=0, tiled=True)


def spread_slices(rows, count, width):
    own = lax.axis_index("occ")
    whole = jnp.zeros((count, rows.shape[0], width), rows.dtype)
    for step in range(count):
        peer = own ^ step
        piece = lax.dynamic_slice_in_dim(rows, peer * width, width, 1)
        if step:
            piece = lax.ppermute(piece, "occ", [(i, i ^ step) for i in range(count)])
        whole = lax.dynamic_update_index_in_dim(whole, piece, peer, 0)
    return whole


def on_device(amplitudes, left_factor, right_factor, other_terms):
    occ_count = lax.axis_size("occ")
    aux_count = lax.axis_size("aux")
    sec_count = lax.axis_size(VSEC)
    plane_count = aux_count * sec_count
    aux_rows, arow_count, virt_width = left_factor.shape
    window, slice_width = right_factor.shape[1:]
    sub = virt_width // plane_count
    per_device = other_terms.shape[0]

    amps = amplitudes.reshape(sec_count, sub, occ_count * slice_width)
    amps = exchange(amps, VSEC).reshape(sec_count * sub, occ_count * slice_width)

    partial = lax.dot_general(
        left_factor, right_factor, (((0,), (0,)), ((), ())), preferred_element_type=jnp.float32
    )
    partial = (partial * SCALE).astype(jnp.float16)
    partial = partial.reshape(arow_count, plane_count, sub, window, slice_width)
    partial = jnp.transpose(partial, (1, 0, 3, 2, 4))
    partial, amps = lax.optimization_barrier((partial, amps))
    arrived = exchange(partial, PLANE)
    amps = spread_slices(amps, occ_count, slice_width)
    amps = amps.reshape(occ_count * sec_count, sub, slice_width)
    halves = arrived.reshape(aux_count, sec_count * arow_count, window, sub, slice_width)
    total = halves[0].astype(jnp.float32)
    for half in range(1, aux_count):
        total = total + halves[half].astype(jnp.float32)
    integral = (total * (1.0 / SCALE)).astype(jnp.bfloat16)

    rows = arow_count * window
    pairs = amps.shape[0]
    place = lax.axis_index(OCC_AUX) * per_device
    others = jnp.transpose(other_terms.reshape(per_device, rows))
    others = lax.dynamic_update_slice(jnp.zeros((rows, pairs), jnp.float32), others, (0, place))
    integral, others = lax.optimization_barrier((integral, others))
    ladder = lax.dot_general(
        integral, amps, (((2, 3), (1, 2)), ((), ())), preferred_element_type=jnp.float32
    )
    mine = exchange(ladder.reshape(sec_count, rows, pairs), VSEC).sum(axis=0)
    mine = mine + others
    spread = jnp.broadcast_to(mine, (occ_count * aux_count, rows, pairs))
    whole = exchange(spread, OCC_AUX).sum(axis=0)
    residual = lax.dynamic_slice_in_dim(whole, place, per_device, 1)
    residual = jnp.transpose(residual).reshape(other_terms.shape)
    square = jnp.sum(whole * whole, axis=0)
    square, residual = lax.optimization_barrier((square, residual))
    squares = exchange(jnp.broadcast_to(square, (sec_count, 1, pairs)), VSEC)
    norm = jnp.sqrt(jnp.sum(squares))
    return (residual, norm)


def solution(mesh):
    torus = Mesh(
        mesh.devices.reshape(mesh.shape["occ"], 4, 2, 2, mesh.shape["aux"]),
        ("occ", "vsec_0", "vsec_1", "vsec_2", "aux"),
    )
    in_specs = (
        P(OCC_VSEC, "aux", None),
        P("aux", VSEC, None),
        P("aux", None, "occ"),
        P(("occ", "aux"), VSEC, None),
    )
    out_specs = (P(("occ", "aux"), VSEC, None), P())
    return jax.shard_map(
        on_device, mesh=torus, in_specs=in_specs, out_specs=out_specs, check_vma=False
    )
```

```python
import jax
import jax.numpy as jnp
from jax import lax
from jax.sharding import Mesh
from jax.sharding import PartitionSpec as P

VSEC = ("vsec_0", "vsec_1", "vsec_2")
SECTIONS = VSEC[::-1]
PLANE = ("aux",) + SECTIONS
OCC_VSEC = ("occ",) + VSEC
OCC_AUX = ("occ", "aux")
SCALE = 32.0


def exchange(x, axes):
    return lax.all_to_all(x, axes, split_axis=0, concat_axis=0, tiled=True)


def spread_slices(rows, count, width):
    own = lax.axis_index("occ")
    whole = jnp.zeros((count, rows.shape[0], width), rows.dtype)
    for step in range(count):
        peer = own ^ step
        piece = lax.dynamic_slice_in_dim(rows, peer * width, width, 1)
        if step:
            piece = lax.ppermute(piece, "occ", [(i, i ^ step) for i in range(count)])
        whole = lax.dynamic_update_index_in_dim(whole, piece, peer, 0)
    return whole


def on_device(amplitudes, left_factor, right_factor, other_terms):
    occ_count = lax.axis_size("occ")
    aux_count = lax.axis_size("aux")
    sec_count = lax.axis_size(VSEC)
    plane_count = aux_count * sec_count
    aux_rows, arow_count, virt_width = left_factor.shape
    window, slice_width = right_factor.shape[1:]
    sub = virt_width // plane_count
    per_device = other_terms.shape[0]

    amps = amplitudes.reshape(sec_count, sub, occ_count * slice_width)
    amps = exchange(amps, VSEC).reshape(sec_count * sub, occ_count * slice_width)

    partial = lax.dot_general(
        left_factor, right_factor, (((0,), (0,)), ((), ())), preferred_element_type=jnp.float32
    )
    partial = (partial * SCALE).astype(jnp.float16)
    sides = [lax.axis_size(axis) for axis in VSEC]
    partial = partial.reshape(arow_count, aux_count, *sides, sub, window, slice_width)
    partial = jnp.transpose(partial, (1, 4, 3, 2, 0, 6, 5, 7))
    partial = partial.reshape(plane_count, arow_count, window, sub, slice_width)
    partial, amps = lax.optimization_barrier((partial, amps))
    arrived = exchange(partial, PLANE)
    amps = spread_slices(amps, occ_count, slice_width)
    amps = amps.reshape(occ_count * sec_count, sub, slice_width)
    halves = arrived.reshape(aux_count, sec_count * arow_count, window, sub, slice_width)
    total = halves[0].astype(jnp.float32)
    for half in range(1, aux_count):
        total = total + halves[half].astype(jnp.float32)
    integral = (total * (1.0 / SCALE)).astype(jnp.bfloat16)

    rows = arow_count * window
    pairs = amps.shape[0]
    place = lax.axis_index(OCC_AUX) * per_device
    others = jnp.transpose(other_terms.reshape(per_device, rows))
    others = lax.dynamic_update_slice(jnp.zeros((rows, pairs), jnp.float32), others, (0, place))
    integral, others = lax.optimization_barrier((integral, others))
    ladder = lax.dot_general(
        integral, amps, (((2, 3), (1, 2)), ((), ())), preferred_element_type=jnp.float32
    )
    mine = exchange(ladder.reshape(sec_count, rows, pairs), SECTIONS).sum(axis=0)
    mine = mine + others
    spread = jnp.broadcast_to(mine, (occ_count * aux_count, rows, pairs))
    whole = exchange(spread, OCC_AUX).sum(axis=0)
    residual = lax.dynamic_slice_in_dim(whole, place, per_device, 1)
    residual = jnp.transpose(residual).reshape(other_terms.shape)
    square = jnp.sum(whole * whole, axis=0)
    square, residual = lax.optimization_barrier((square, residual))
    squares = exchange(jnp.broadcast_to(square, (sec_count, 1, pairs)), VSEC)
    norm = jnp.sqrt(jnp.sum(squares))
    return (residual, norm)


def solution(mesh):
    torus = Mesh(
        mesh.devices.reshape(mesh.shape["occ"], 4, 2, 2, mesh.shape["aux"]),
        ("occ", "vsec_0", "vsec_1", "vsec_2", "aux"),
    )
    in_specs = (
        P(OCC_VSEC, "aux", None),
        P("aux", VSEC, None),
        P("aux", None, "occ"),
        P(("occ", "aux"), VSEC, None),
    )
    out_specs = (P(("occ", "aux"), VSEC, None), P())
    return jax.shard_map(
        on_device, mesh=torus, in_specs=in_specs, out_specs=out_specs, check_vma=False
    )
```
